32 devices in a mesh: tm: 8 (over z, core), dp: 4 (over y, x).
Axes of the slice: x: 2, y: 2, z: 4, core: 2. Of those that a mesh axis runs over, the one named last changes fastest.
Arguments:
- encoded: bfloat16 [512, 80, 1024], P('dp', 'tm'), may hold values from -6 to 6
- queries: bfloat16 [512, 32, 1024], P(('dp', 'tm')), may hold values from -200 to 200
- cotangent: bfloat16 [512, 32, 1024], P(('dp', 'tm')), may hold values from -0.08886719 to 0.08886719
- lengths: int32 [512], P(('dp', 'tm')), may hold values from 2 to 80
- key_weight: bfloat16 [1024, 1024], replicated, may hold values from -0.1875 to 0.1875
- value_weight: bfloat16 [1024, 1024], replicated, may hold values from -0.1875 to 0.1875
Outputs:
- context: bfloat16 [512, 32, 1024], P(('dp', 'tm'))
- key_grad: float32 [1024, 1024], replicated
- value_grad: float32 [1024, 1024], replicated
The draws below stay inside these ranges and needn't reach their ends.
Inputs may be any that keep to these rules, and one draw needn't show every extreme that they name: Sequence b attends only to source positions below lengths[b].
All inputs are finite; a program needn't handle non-finite values.
Results may differ from the reference program's by a relative error of at most 0.0069.
Values may be sent and summed in bfloat16 or wider, within the bound.
No kernel may reach another device: no remote copies, remote signals or barrier semaphores. Data moves between devices by JAX's collectives and lax.ppermute only.
A program may use at most 128 MiB of HBM per device.

```python
import math
import jax
import jax.numpy as jnp
from jax import lax

D = 1024
SRC = 80
TGT = 32
SEQ_DEV = 16
BATCH = 512
N_DP = 4


def encoded_values(key):
    base = jax.random.fold_in(key, 11)
    drawn = jax.random.truncated_normal(base, -6.0, 6.0, (BATCH, SRC, D), jnp.float32)
    return drawn.astype(jnp.bfloat16)


def key_matrix(key):
    base = jax.random.fold_in(key, 12)
    drawn = jax.random.truncated_normal(base, -6.0, 6.0, (D, D), jnp.float32) / math.sqrt(D)
    return drawn.astype(jnp.bfloat16)


def draw_encoded(key, part):
    return encoded_values(key)


def draw_key_weight(key, part):
    return key_matrix(key)


def draw_queries(key, part):
    base = jax.random.fold_in(key, 13)
    drawn = jax.random.truncated_normal(base, -6.0, 6.0, (BATCH, TGT, D), jnp.float32)
    return drawn.astype(jnp.bfloat16)


def place_ends(result, rng, least, high):
    shape = result.shape
    spot = [jax.random.randint(jax.random.fold_in(rng, axis), (), 0, shape[axis]) for axis in range(len(shape))]
    result = result.at[tuple(spot)].set(least)
    longest = shape.index(max(shape))
    spot[longest] = (spot[longest] + 1) % shape[longest]
    return result.at[tuple(spot)].set(high)


def level_of(rng, extent, shards, smallest, high):
    def one(position, blocks):
        heights = jax.random.uniform(jax.random.fold_in(jax.random.fold_in(rng, 6), position), (blocks,), jnp.float32, smallest / len(shards), high / len(shards))
        return jnp.repeat(jnp.exp(heights), extent[position] // blocks).reshape((-1,) + (1,) * (len(extent) - position - 1))

    gain = one(*shards[0])
    for cut in shards[1:]:
        gain = gain * one(*cut)
    return gain


def normal_values(stream_key, shape, deviation, bound, split=(), kind=jnp.bfloat16):
    entries = jax.random.normal(stream_key, shape, jnp.float32) * deviation
    if len(split) > 0:
        entries = level_of(stream_key, shape, split, -0.22, 0.18) * entries
    return jnp.clip(entries, min=-bound, max=bound).astype(kind)


def setup_inputs(seed: int = 0) -> dict:
    seeds = jax.random.split(jax.random.key(seed), 7)
    encoded = draw_encoded(jax.random.fold_in(seeds[6], 71), 0)
    queries = draw_queries(jax.random.fold_in(seeds[6], 71), 0)
    cotangent = normal_values(seeds[2], (BATCH, TGT, D), (3.0 / (BATCH * SRC) ** 0.5), 0.08886719, ((0, 32),))
    lengths = place_ends(jax.random.randint(seeds[3], (BATCH,), 2, SRC + 1), jax.random.fold_in(seeds[3], 1), 2, SRC).astype(jnp.int32)
    key_weight = draw_key_weight(jax.random.fold_in(seeds[6], 71), 0)
    value_weight = normal_values(seeds[5], (D, D), D ** -0.5, 0.1875)
    return dict(encoded=encoded, queries=queries, cotangent=cotangent, lengths=lengths, key_weight=key_weight, value_weight=value_weight)


def attend(queries, key_rows, value_rows, lengths, cotangent):
    score_scale = 1.0 / math.sqrt(queries.shape[-1])
    scores = jnp.einsum('btd,bsd->bts', queries.astype(jnp.float32), key_rows.astype(jnp.float32)) * score_scale
    positions = jnp.arange(key_rows.shape[1], dtype=jnp.int32)
    in_range = positions[None, None, :] < lengths[:, None, None]
    scores = jnp.where(in_range, scores, -1e+30)
    row_max = lax.optimization_barrier(jnp.max(scores, axis=-1, keepdims=True))
    weights = jnp.exp(scores - row_max)
    probabilities = weights / lax.optimization_barrier(jnp.sum(weights, axis=-1, keepdims=True))
    probs_low = lax.optimization_barrier(probabilities.astype(jnp.bfloat16))
    context = jnp.einsum('bts,bsd->btd', probs_low.astype(jnp.float32), value_rows.astype(jnp.float32)).astype(jnp.bfloat16)
    grad_probs = jnp.einsum('btd,bsd->bts', cotangent.astype(jnp.float32), value_rows.astype(jnp.float32))
    grad_scores = probabilities * (grad_probs - lax.optimization_barrier(jnp.sum(probabilities * grad_probs, axis=-1, keepdims=True)))
    grad_low = lax.optimization_barrier(grad_scores.astype(jnp.bfloat16))
    grad_values = jnp.einsum('bts,btd->bsd', probs_low.astype(jnp.float32), cotangent.astype(jnp.float32)).astype(jnp.bfloat16)
    grad_keys = (jnp.einsum('bts,btd->bsd', grad_low.astype(jnp.float32), queries.astype(jnp.float32)) * score_scale).astype(jnp.bfloat16)
    return (context, grad_keys, grad_values)

def reference(encoded, queries, cotangent, lengths, key_weight, value_weight):
    block_rows = SEQ_DEV * N_DP
    block_count = BATCH // block_rows
    enc_blocks = encoded.reshape(block_count, block_rows, SRC, D)
    query_blocks = queries.reshape(block_count, block_rows, TGT, D)
    cotan_blocks = cotangent.reshape(block_count, block_rows, TGT, D)
    length_blocks = lengths.reshape(block_count, block_rows)

    def scan_step(totals, pieces):
        enc_block, query_block, cotan_block, length_block = pieces
        flattened = enc_block.reshape(-1, D)
        key_rows = jnp.dot(flattened, key_weight, preferred_element_type=jnp.float32).astype(jnp.bfloat16).reshape(block_rows, SRC, D)
        value_rows = jnp.dot(flattened, value_weight, preferred_element_type=jnp.float32).astype(jnp.bfloat16).reshape(block_rows, SRC, D)
        context, grad_keys, grad_values = attend(query_block, key_rows, value_rows, length_block, cotan_block)
        key_total = totals[0] + jnp.dot(flattened.T, grad_keys.reshape(-1, D), preferred_element_type=jnp.float32)
        value_total = totals[1] + jnp.dot(flattened.T, grad_values.reshape(-1, D), preferred_element_type=jnp.float32)
        return ((key_total, value_total), context)
    zeros = jnp.zeros((D, D), jnp.float32)
    totals, contexts = lax.scan(scan_step, (zeros, zeros), (enc_blocks, query_blocks, cotan_blocks, length_blocks))
    return (contexts.reshape(BATCH, TGT, D), totals[0], totals[1])
```

```python
import math

import jax
import jax.numpy as jnp
from jax import lax
from jax.sharding import PartitionSpec as P

F32, BF16 = jnp.float32, jnp.bfloat16


def swap(x, axis, size, k):
    return lax.ppermute(x, axis, [(i, i ^ k) for i in range(size)])


def pick(x, index):
    return lax.dynamic_index_in_dim(x, index, 0, keepdims=False)


def unscramble(x, me):
    n, bit = x.shape[0], 1
    while bit < n:
        y = x.reshape((n // (2 * bit), 2, bit) + x.shape[1:])
        y = jnp.where((me & bit) != 0, y[:, ::-1], y)
        x, bit = y.reshape(x.shape), bit * 2
    return x


def regroup(encoded, n_tm):
    me = lax.axis_index("tm")
    moved = jnp.transpose(encoded, (1, 0, 2))
    own_pos, seqs, width = moved.shape
    count = seqs // n_tm
    order = [k for k in range(n_tm - 1, 0, -1)]
    blocks = {}
    for k in order:
        out = lax.dynamic_slice_in_dim(moved, (me ^ k) * count, count, axis=1)
        blocks[k] = swap(out, "tm", n_tm, k)
    blocks[0] = lax.dynamic_slice_in_dim(moved, me * count, count, axis=1)
    stacked = jnp.stack([blocks[k] for k in range(n_tm)])
    return unscramble(stacked, me).reshape(n_tm * own_pos, count, width)


def sum_all(partial, n_tm, n_dp):
    me, dp = lax.axis_index("tm"), lax.axis_index("dp")
    core, chip = me & 1, me >> 1
    n_z, width = n_tm // 2, partial.shape[1]
    rows = partial.shape[0] // (n_tm * n_dp)
    halves = partial.reshape(2, -1, width)
    other = swap(pick(halves, 1 - core).astype(BF16), "tm", n_tm, 1)
    total = pick(halves, core) + other.astype(F32)
    blocks = total.reshape(n_dp, n_z * rows, width)
    got = [swap(pick(blocks, dp ^ k).astype(BF16), "dp", n_dp, k) for k in range(1, n_dp)]
    total = pick(blocks, dp)
    for g in got:
        total = total + g.astype(F32)
    shards = total.reshape(n_z, rows, width)
    got = [swap(pick(shards, chip ^ k).astype(BF16), "tm", n_tm, 2 * k) for k in range(1, n_z)]
    total = pick(shards, chip)
    for g in got:
        total = total + g.astype(F32)
    mine = total.astype(BF16)
    column = jnp.stack([mine] + [swap(mine, "tm", n_tm, 2 * k) for k in range(1, n_z)])
    plane = [column] + [swap(column, "dp", n_dp, k) for k in range(1, n_dp)]
    half = jnp.stack(plane)
    both = jnp.stack([half, swap(half, "tm", n_tm, 1)])
    both = unscramble(both, core)
    both = jnp.moveaxis(unscramble(jnp.moveaxis(both, 1, 0), dp), 0, 1)
    both = jnp.moveaxis(unscramble(jnp.moveaxis(both, 2, 0), chip), 0, 2)
    return both.reshape(partial.shape).astype(F32)


def attend(queries, key_rows, value_rows, lengths, cotangent):
    score_scale = 1.0 / math.sqrt(queries.shape[-1])
    scores = jnp.einsum("btd,bsd->bts", queries, key_rows, preferred_element_type=F32) * score_scale
    positions = jnp.arange(key_rows.shape[1], dtype=jnp.int32)
    in_range = positions[None, None, :] < lengths[:, None, None]
    scores = jnp.where(in_range, scores, -1e30)
    row_max = jnp.max(scores, axis=-1, keepdims=True)
    weights = jnp.exp(scores - row_max)
    probs = weights / jnp.sum(weights, axis=-1, keepdims=True)
    probs_low = probs.astype(BF16)
    context = jnp.einsum("bts,bsd->btd", probs_low, value_rows, preferred_element_type=F32).astype(BF16)
    grad_probs = jnp.einsum("btd,bsd->bts", cotangent, value_rows, preferred_element_type=F32)
    grad_scores = probs * (grad_probs - jnp.sum(probs * grad_probs, axis=-1, keepdims=True))
    grad_low = grad_scores.astype(BF16)
    grad_values = jnp.einsum("bts,btd->bsd", probs_low, cotangent, preferred_element_type=F32).astype(BF16)
    grad_keys = (jnp.einsum("bts,btd->bsd", grad_low, queries, preferred_element_type=F32) * score_scale).astype(BF16)
    return context, grad_keys, grad_values


def weight_term(flattened, gradient):
    width = flattened.shape[1]
    return lax.dot_general(
        flattened, gradient.reshape(-1, width), (((0,), (0,)), ((), ())), preferred_element_type=F32
    )


def solution(mesh):
    n_tm, n_dp = mesh.shape["tm"], mesh.shape["dp"]

    def body(encoded, queries, cotangent, lengths, key_weight, value_weight):
        regrouped = jnp.transpose(regroup(encoded, n_tm), (1, 0, 2))
        shape = regrouped.shape
        flattened = regrouped.reshape(-1, shape[2])
        key_rows = jnp.dot(flattened, key_weight, preferred_element_type=F32).astype(BF16).reshape(shape)
        value_rows = jnp.dot(flattened, value_weight, preferred_element_type=F32).astype(BF16).reshape(shape)
        context, grad_keys, grad_values = attend(queries, key_rows, value_rows, lengths, cotangent)
        value_grad = sum_all(weight_term(flattened, grad_values), n_tm, n_dp)
        key_grad = sum_all(weight_term(flattened, grad_keys), n_tm, n_dp)
        return context, key_grad, value_grad

    seqs = P(("dp", "tm"), None, None)
    return jax.shard_map(
        body,
        mesh=mesh,
        in_specs=(P("dp", "tm", None), seqs, seqs, P(("dp", "tm")), P(), P()),
        out_specs=(seqs, P(), P()),
        check_vma=False,
    )
```

```python
import functools
import math

import jax
import jax.numpy as jnp
from jax import lax
from jax.experimental import pallas as pl
from jax.experimental.pallas import tpu as pltpu
from jax.sharding import PartitionSpec as P


F32, BF16 = jnp.float32, jnp.bfloat16
CHUNKS = 2
FRONT_MIB = 56
BACK_MIB = 56
LANES = 256


def swap(x, axis, size, k):
    return lax.ppermute(x, axis, [(i, i ^ k) for i in range(size)])


def pick(x, index):
    return lax.dynamic_index_in_dim(x, index, 0, keepdims=False)


def dot(a, b, contract):
    return lax.dot_general(a, b, (contract, ((), ())), preferred_element_type=F32)


def params(mib):
    return pltpu.CompilerParams(vmem_limit_bytes=mib * 1024 * 1024)


def vmem(n):
    return [pl.BlockSpec(memory_space=pltpu.VMEM)] * n


def smem(n):
    return [pl.BlockSpec(memory_space=pltpu.SMEM)] * n


def cost(flops, nbytes):
    return pl.CostEstimate(flops=int(flops), bytes_accessed=int(nbytes), transcendentals=0)


def spaces(n):
    return [pl.BlockSpec(memory_space=pl.ANY)] * n


def loader(sem):
    count = [0]

    def start(src, dst):
        copy = pltpu.make_async_copy(src, dst, sem.at[count[0]])
        count[0] += 1
        copy.start()
        return copy

    return start


def own_block(full_ref, count, src, tgt):
    lane = lax.broadcasted_iota(jnp.int32, (src, count * tgt), 1) // tgt
    out = jnp.zeros((src, count * tgt), F32)
    for b in range(count):
        out = jnp.where(lane == b, full_ref[b * src : (b + 1) * src, :], out)
    return out


def spread(low, diag_ref, count, src, tgt):
    lane = lax.broadcasted_iota(jnp.int32, (src, count * tgt), 1) // tgt
    for b in range(count):
        diag_ref[b * src : (b + 1) * src, :] = jnp.where(lane == b, low, 0.0).astype(BF16)


def product(a_ref, b_ref, out_ref, scale=None):
    for n in range(b_ref.shape[1] // LANES):
        cols = slice(n * LANES, (n + 1) * LANES)
        part = dot(a_ref[...], b_ref[:, cols], ((1,), (0,)))
        out_ref[:, cols] = (part if scale is None else part * scale).astype(out_ref.dtype)


def half_term(pairs, out_ref, send):
    copies = []
    for n in range(out_ref.shape[1] // LANES):
        cols = slice(n * LANES, (n + 1) * LANES)
        total = None
        for a_ref, b_ref in pairs:
            part = dot(a_ref[...], b_ref[:, cols], ((1,), (0,)))
            total = part if total is None else total + part
        out_ref[:, cols] = total.astype(out_ref.dtype)
        copies.append(send(cols))
    return copies


def front_kernel(n_src, own_pos, count, src, tgt, chunk, tail, me_ref, half_ref, len_ref, *refs):
    blocks, refs = refs[:n_src], refs[n_src:]
    (q_in, c_in, wk_in), refs = refs[:3], refs[3:]
    if tail:
        (etp_in, gvp_in), refs = refs[:2], refs[2:]
    (e_out, et_out, p_ref, gv_out), refs = refs[:4], refs[4:]
    if tail:
        vo_out, refs = refs[0], refs[1:]
    in_ref, q_ref, c_ref, wk_ref, e_ref, et_ref, k_ref, full_ref, diag_ref, gv_ref, sem = refs[:11]
    width, step, bt, rows_in = wk_ref.shape[0], 16, count * tgt, own_pos * count
    half = width // 2
    start = loader(sem)
    got = [start(ref, in_ref.at[k]) for k, ref in enumerate(blocks)]
    here = pl.ds(chunk * bt, bt)
    got_wk = start(wk_in, wk_ref)
    got_q = start(q_in.at[here], q_ref)
    got_c = start(c_in.at[here], c_ref)
    if tail:
        etp_ref, gvp_ref, eth_ref, vo_ref = refs[11:]
        top = pl.ds(pl.multiple_of(half_ref[0] * half, half), half)
        got_tail = [start(etp_in.at[top], etp_ref), start(gvp_in, gvp_ref)]
    me = me_ref[0]
    for copy in got:
        copy.wait()
    for j in range(src // step):
        lo, hi = j * step, (j + 1) * step
        out = None
        for k in range(lo // own_pos, (hi - 1) // own_pos + 1):
            r = lax.broadcasted_iota(jnp.int32, (step * count, rows_in), 0)
            c = lax.broadcasted_iota(jnp.int32, (step * count, rows_in), 1)
            want = (lo + r % step - k * own_pos) * count + r // step
            hot = jnp.where(c == want, 1.0, 0.0).astype(BF16)
            term = dot(hot, in_ref[k], ((1,), (0,)))
            out = term if out is None else out + term
        out = out.astype(BF16)
        for b in range(count):
            e_ref[b * src + lo : b * src + hi, :] = out[b * step : (b + 1) * step]
    sent = [start(e_ref, e_out)]
    got_wk.wait()
    product(e_ref, wk_ref, k_ref)
    got_q.wait()
    full_ref[...] = dot(k_ref[...], q_ref[...], ((1,), (1,)))
    for n in range(width // LANES):
        cols = slice(n * LANES, (n + 1) * LANES)
        et_ref[cols, :] = e_ref[:, cols].T
    sent.append(start(et_ref, et_out))
    rel = lax.broadcasted_iota(jnp.int32, (src, bt), 0)
    place = (me ^ (rel // own_pos)) * own_pos + rel % own_pos
    scores = own_block(full_ref, count, src, tgt) * (1.0 / math.sqrt(width))
    scores = jnp.where(place < len_ref[:, chunk * bt : (chunk + 1) * bt], scores, -1e30)
    weights = jnp.exp(scores - jnp.max(scores, axis=0, keepdims=True))
    probs = weights / jnp.sum(weights, axis=0, keepdims=True)
    p_ref[...] = probs
    spread(probs.astype(BF16).astype(F32), diag_ref, count, src, tgt)
    got_c.wait()
    product(diag_ref, c_ref, gv_ref)
    sent.append(start(gv_ref, gv_out))
    if tail:
        for copy in got_tail:
            copy.wait()
        eth_ref[...] = et_ref[top, :]
        sent += half_term(
            ((etp_ref, gvp_ref), (eth_ref, gv_ref)), vo_ref,
            lambda cols: start(vo_ref.at[:, cols], vo_out.at[:, cols]),
        )
    for copy in sent:
        copy.wait()


def front(me, half, lens, blocks, queries, cotangent, key_weight, own_pos, src, tgt, chunk, before):
    n, width = len(blocks), queries.shape[1]
    count = blocks[0].shape[0] // own_pos
    rows, bt = count * src, count * tgt
    tail = before is not None
    shape = lambda *dims, dtype=BF16: jax.ShapeDtypeStruct(dims, dtype)
    outs = [shape(rows, width), shape(width, rows), shape(src, bt, dtype=F32), shape(rows, width)]
    scratch = [
        pltpu.VMEM((n,) + blocks[0].shape, BF16),
        pltpu.VMEM((bt, width), BF16),
        pltpu.VMEM((bt, width), BF16),
        pltpu.VMEM((width, width), BF16),
        pltpu.VMEM((rows, width), BF16),
        pltpu.VMEM((width, rows), BF16),
        pltpu.VMEM((rows, width), BF16),
        pltpu.VMEM((rows, bt), F32),
        pltpu.VMEM((rows, bt), BF16),
        pltpu.VMEM((rows, width), BF16),
        pltpu.SemaphoreType.DMA((n + 16,)),
    ]
    if tail:
        outs.append(shape(width // 2, width))
        scratch += [
            pltpu.VMEM((width // 2, rows), BF16),
            pltpu.VMEM((rows, width), BF16),
            pltpu.VMEM((width // 2, rows), BF16),
            pltpu.VMEM((width // 2, width), BF16),
        ]
    return pl.pallas_call(
        functools.partial(front_kernel, n, own_pos, count, src, tgt, chunk, tail),
        out_shape=tuple(outs),
        in_specs=smem(2) + vmem(1) + spaces(n + 3 + 2 * tail),
        out_specs=tuple(spaces(2) + vmem(1) + spaces(1 + tail)),
        scratch_shapes=scratch,
        compiler_params=params(FRONT_MIB),
        cost_estimate=cost(4 * rows * width * width, 12 * width * width),
        name="front",
    )(me, half, lens, *blocks, queries, cotangent, key_weight, *(before or ()))


def back_kernel(count, src, tgt, chunk, tail, half_ref, p_ref, *refs):
    (e_in, q_in, c_in, wv_in), refs = refs[:4], refs[4:]
    if tail:
        (etp_in, gkp_in, etc_in, _), refs = refs[:4], refs[4:]
    (ctx_out, gk_out), refs = refs[:2], refs[2:]
    if tail:
        ko_out, refs = refs[0], refs[1:]
    e_ref, q_ref, c_ref, wv_ref, v_ref, full_ref, diag_ref, pdiag_ref, gk_ref, ctx_ref, sem = refs[:11]
    width, bt = wv_ref.shape[0], count * tgt
    half = width // 2
    start = loader(sem)
    here = pl.ds(chunk * bt, bt)
    got = [start(e_in, e_ref), start(wv_in, wv_ref)]
    got_c = start(c_in.at[here], c_ref)
    got_q = start(q_in.at[here], q_ref)
    if tail:
        etp_ref, gkp_ref, etc_ref, ko_ref = refs[11:]
        top = pl.ds(pl.multiple_of(half_ref[0] * half, half), half)
        got_tail = [start(etp_in.at[top], etp_ref), start(gkp_in, gkp_ref), start(etc_in.at[top], etc_ref)]
    for copy in got:
        copy.wait()
    product(e_ref, wv_ref, v_ref)
    got_c.wait()
    full_ref[...] = dot(v_ref[...], c_ref[...], ((1,), (1,)))
    probs = p_ref[...]
    grad_probs = own_block(full_ref, count, src, tgt)
    mean = jnp.sum(probs * grad_probs, axis=0, keepdims=True)
    low = (probs * (grad_probs - mean)).astype(BF16).astype(F32)
    spread(low, diag_ref, count, src, tgt)
    got_q.wait()
    product(diag_ref, q_ref, gk_ref, 1.0 / math.sqrt(width))
    sent = [start(gk_ref, gk_out)]
    if tail:
        for copy in got_tail:
            copy.wait()
        sent += half_term(
            ((etp_ref, gkp_ref), (etc_ref, gk_ref)), ko_ref,
            lambda cols: start(ko_ref.at[:, cols], ko_out.at[:, cols]),
        )
    spread(probs.astype(BF16).astype(F32), pdiag_ref, count, src, tgt)
    for n in range(width // LANES):
        cols = slice(n * LANES, (n + 1) * LANES)
        ctx_ref[:, cols] = dot(pdiag_ref[...], v_ref[:, cols], ((0,), (0,))).astype(BF16)
    sent.append(start(ctx_ref, ctx_out.at[here]))
    for copy in sent:
        copy.wait()


def back(half, probs, rows_e, queries, cotangent, value_weight, tgt, chunk, before):
    src, bt = probs.shape
    rows, width = rows_e.shape
    tail = before is not None
    outs = [jax.ShapeDtypeStruct(queries.shape, BF16), jax.ShapeDtypeStruct((rows, width), BF16)]
    scratch = [
        pltpu.VMEM((rows, width), BF16),
        pltpu.VMEM((bt, width), BF16),
        pltpu.VMEM((bt, width), BF16),
        pltpu.VMEM((width, width), BF16),
        pltpu.VMEM((rows, width), BF16),
        pltpu.VMEM((rows, bt), F32),
        pltpu.VMEM((rows, bt), BF16),
        pltpu.VMEM((rows, bt), BF16),
        pltpu.VMEM((rows, width), BF16),
        pltpu.VMEM((bt, width), BF16),
        pltpu.SemaphoreType.DMA((24,)),
    ]
    if tail:
        outs.append(jax.ShapeDtypeStruct((width // 2, width), BF16))
        scratch += [
            pltpu.VMEM((width // 2, rows), BF16),
            pltpu.VMEM((rows, width), BF16),
            pltpu.VMEM((width // 2, rows), BF16),
            pltpu.VMEM((width // 2, width), BF16),
        ]
    return pl.pallas_call(
        functools.partial(back_kernel, bt // tgt, src, tgt, chunk, tail),
        out_shape=tuple(outs),
        in_specs=smem(1) + vmem(1) + spaces(4 + 4 * tail),
        out_specs=tuple(spaces(2 + tail)),
        input_output_aliases={9: 0} if tail else {},
        scratch_shapes=scratch,
        compiler_params=params(BACK_MIB),
        cost_estimate=cost(4 * rows * width * width, 12 * width * width),
        name="back",
    )(half, probs, rows_e, queries, cotangent, value_weight, *(before or ()))


def term_kernel(n, half_ref, *refs):
    rows, grads, out_ref = refs[:n], refs[n : 2 * n], refs[2 * n]
    half = out_ref.shape[0]
    tall = pl.ds(pl.multiple_of(half_ref[0] * half, half), half)
    for j in range(out_ref.shape[1] // LANES):
        lanes = slice(j * LANES, (j + 1) * LANES)
        total = None
        for e_ref, g_ref in zip(rows, grads):
            part = dot(e_ref[tall, :], g_ref[:, lanes], ((1,), (0,)))
            total = part if total is None else total + part
        out_ref[:, lanes] = total.astype(out_ref.dtype)


def term(half, rows, grads, dtype):
    n, width = len(rows), rows[0].shape[0]
    return pl.pallas_call(
        functools.partial(term_kernel, n),
        out_shape=jax.ShapeDtypeStruct((width // 2, width), dtype),
        in_specs=smem(1) + vmem(2 * n),
        out_specs=vmem(1)[0],
        compiler_params=params(20),
        cost_estimate=cost(n * rows[0].shape[1] * width * width, 4 * width * width),
        name="term",
    )(half, *rows, *grads)


def join_kernel(n, size, code_ref, *refs):
    pieces, out_ref = refs[:-1], refs[-1]
    for i, ref in enumerate(pieces):
        piece = ref[...].astype(F32)
        for k in range(n):
            at = pl.multiple_of(((i * n + k) ^ code_ref[0]) * size, size)
            out_ref[pl.ds(at, size), :] = piece[k * size : (k + 1) * size]


def join(code, pieces, n):
    tall, width = pieces[0].shape
    return pl.pallas_call(
        functools.partial(join_kernel, n, tall // n),
        out_shape=jax.ShapeDtypeStruct((tall * len(pieces), width), F32),
        in_specs=smem(1) + vmem(len(pieces)),
        out_specs=vmem(1)[0],
        compiler_params=params(12),
        cost_estimate=cost(tall * width * 64, 6 * tall * len(pieces) * width),
        name="join",
    )(code, *pieces)


def sum_all(other, own, n_tm, n_dp):
    me, dp = lax.axis_index("tm"), lax.axis_index("dp")
    core, chip = me & 1, me >> 1
    n_z, width = n_tm // 2, own.shape[1]
    size = own.shape[0] // (n_z * n_dp)
    came = swap(other, "tm", n_tm, 1)
    blocks = (own + came.astype(F32)).reshape(n_dp, n_z * size, width)
    got = [swap(pick(blocks, dp ^ k).astype(BF16), "dp", n_dp, k) for k in range(n_dp - 1, 0, -1)]
    total = pick(blocks, dp)
    for g in got:
        total = total + g.astype(F32)
    shards = total.reshape(n_z, size, width)
    got = [swap(pick(shards, chip ^ k).astype(BF16), "tm", n_tm, 2 * k) for k in range(n_z - 1, 0, -1)]
    total = pick(shards, chip)
    for g in got:
        total = total + g.astype(F32)
    mine = total.astype(BF16)
    column = [mine] + [swap(mine, "tm", n_tm, 2 * k) for k in range(1, n_z)]
    column = jnp.concatenate(column, axis=0)
    plane = [column] + [swap(column, "dp", n_dp, k) for k in range(1, n_dp)]
    both = plane + [swap(piece, "tm", n_tm, 1) for piece in plane]
    code = ((core * n_dp + dp) * n_z + chip).astype(jnp.int32).reshape(1)
    return join(code, both, n_z)


def solution(mesh):
    n_tm, n_dp = mesh.shape["tm"], mesh.shape["dp"]

    def inner(encoded, queries, cotangent, lengths, key_weight, value_weight):
        me = lax.axis_index("tm")
        moved = jnp.transpose(encoded, (1, 0, 2))
        own_pos, width = moved.shape[0], moved.shape[2]
        src, seqs = n_tm * own_pos, queries.shape[0]
        count = seqs // CHUNKS
        tgt = queries.shape[1]
        index = me.astype(jnp.int32).reshape(1)
        core = (me & 1).astype(jnp.int32).reshape(1)
        q_flat, c_flat = queries.reshape(-1, width), cotangent.reshape(-1, width)
        lens = jnp.repeat(lengths, tgt).reshape(1, -1)
        blocks = []
        for h in range(CHUNKS):
            part = [None] * n_tm
            for k in range(n_tm - 1, -1, -1):
                out = lax.dynamic_slice_in_dim(moved, (me ^ k) * seqs + h * count, count, axis=1)
                out = swap(out, "tm", n_tm, k) if k else out
                part[k] = out.reshape(-1, width)
            blocks.append(part)
        ets, gvs, gks, mid = [], [], [], []
        for h in range(CHUNKS):
            e, et, p, gv, *rest = front(
                index, 1 - core, lens, blocks[h], q_flat, c_flat, key_weight, own_pos, src, tgt, h,
                (ets[0], gvs[0]) if h else None,
            )
            ets.append(et)
            gvs.append(gv)
            mid.append((e, p))
        v_other = rest[0]
        ctx = None
        for h in range(CHUNKS):
            e, p = mid[h]
            ctx, gk, *rest = back(
                1 - core, p, e, q_flat, c_flat, value_weight, tgt, h,
                (ets[0], gks[0], ets[1], ctx) if h else None,
            )
            gks.append(gk)
        k_other = rest[0]
        v_own = term(core, ets, gvs, F32)
        k_own = term(core, ets, gks, F32)
        value_grad = sum_all(v_other, v_own, n_tm, n_dp)
        key_grad = sum_all(k_other, k_own, n_tm, n_dp)
        return ctx.reshape(queries.shape), key_grad, value_grad

    per_seq = P(("dp", "tm"), None, None)
    return jax.shard_map(
        inner,
        mesh=mesh,
        in_specs=(P("dp", "tm", None), per_seq, per_seq, P(("dp", "tm")), P(), P()),
        out_specs=(per_seq, P(), P()),
        check_vma=False,
    )
```
